32 devices in a mesh: gx: 8 (over z, core), gz: 4 (over y, x).
Axes of the slice: x: 2, y: 2, z: 4, core: 2. Of those that a mesh axis runs over, the one named last changes fastest.
Arguments:
- populations: float32 [19, 8, 32, 1024], P(None, None, 'gz', 'gx'), may hold values from 0.001 to 0.6, as said below
- solid: int32 [8, 32, 1024], P(None, 'gz', 'gx'), may hold values from 0 to 1, as said below
- top_inflow: float32 [5, 32, 1024], P(None, 'gz', 'gx'), may hold values from 0.005 to 0.1
Outputs:
- advanced: float32 [19, 8, 32, 1024], P(None, None, 'gz', 'gx')
The draws below stay inside these ranges and needn't reach their ends.
Inputs may be any that keep to these rules, and one draw needn't show every extreme that they name: Positive populations near equilibrium. Only the two planes nearest the wall hold solid nodes.
All inputs are finite; a program needn't handle non-finite values.
Results may differ from the reference program's by a relative error of at most 0.0003.
Values sent between devices are 32-bit elements; how exact they have to be, the bound alone decides.
A program may use at most 64 MiB of HBM per device.

```python
from functools import reduce
import jax
import jax.numpy as jnp
import numpy as np
from jax import lax

NY = 8
STEPS = 2
NX = 1024
NZ = 32


draw_lattice = np.array([[0, 0, 0], [1, 0, 0], [-1, 0, 0], [0, 1, 0], [0, -1, 0], [0, 0, 1], [0, 0, -1], [1, 1, 0], [-1, -1, 0], [1, -1, 0], [-1, 1, 0], [1, 0, 1], [-1, 0, -1], [1, 0, -1], [-1, 0, 1], [0, 1, 1], [0, -1, -1], [0, 1, -1], [0, -1, 1]])


draw_weights = [1.0 / 3.0] + [1.0 / 18.0] * 6 + [1.0 / 36.0] * 12


draw_modes = [(1, 0), (2, 0), (3, 0), (0, 1), (1, 1), (2, 1), (1, 2)]


def draw_equilibrium(density, velocity):
    speed_square = velocity[0] * velocity[0] + velocity[1] * velocity[1] + velocity[2] * velocity[2]
    terms = []
    for index in range(19):
        along = float(draw_lattice[index, 0]) * velocity[0] + float(draw_lattice[index, 1]) * velocity[1] + float(draw_lattice[index, 2]) * velocity[2]
        terms.append(draw_weights[index] * density * (1.0 + 3.0 * along + 4.5 * along * along - 1.5 * speed_square))
    return jnp.stack(terms)


def draw_populations(key, part):
    subkeys = jax.random.split(jax.random.fold_in(key, 11), 8)
    grid_shape = (NY, NZ, NX)
    position = lax.broadcasted_iota(jnp.float32, grid_shape, 2) / float(NX)
    across = lax.broadcasted_iota(jnp.float32, grid_shape, 1) / float(NZ)
    phases = jax.random.uniform(subkeys[6], (len(draw_modes),), jnp.float32, 0.0, 2.0 * np.pi)
    offset = jax.random.uniform(subkeys[7], (), jnp.float32, 0.02, 0.05)
    amplitudes = 0.012 * jax.random.normal(subkeys[5], (len(draw_modes),), jnp.float32)
    regional = jnp.zeros(grid_shape, jnp.float32)
    for mode_index in range(len(draw_modes)):
        wave_x, wave_z = draw_modes[mode_index]
        angle_field = 2.0 * np.pi * (float(wave_x) * position + float(wave_z) * across) + phases[mode_index]
        regional = regional + amplitudes[mode_index] * jnp.cos(angle_field)
    density = 1.0 + 0.04 * jax.random.normal(subkeys[0], grid_shape, jnp.float32)
    speed_x = offset * (1.0 + 2.0 * position) + regional + 0.02 * jax.random.normal(subkeys[1], grid_shape, jnp.float32)
    speed_y = 0.01 * jax.random.normal(subkeys[2], grid_shape, jnp.float32)
    speed_z = 0.02 * jax.random.normal(subkeys[3], grid_shape, jnp.float32)
    fluctuation = 0.05 * jax.random.normal(subkeys[4], (19,) + grid_shape, jnp.float32)
    base_state = draw_equilibrium(density, (speed_x, speed_y, speed_z))
    scaled = jnp.asarray(np.array(draw_weights, dtype=np.float32))[:, None, None, None]
    return jnp.clip(base_state + scaled * fluctuation, 0.001, 0.6).astype(jnp.float32)


def draw_solid(key, part):
    grid_shape = (NY, NZ, NX)
    drawn = jax.random.randint(jax.random.fold_in(key, 23), grid_shape, 0, 100)
    plane = lax.broadcasted_iota(jnp.int32, grid_shape, 0)
    limit = jnp.where(plane == 0, 35, jnp.where(plane == 1, 12, 0))
    return (drawn < limit).astype(jnp.int32)


def draw_top_inflow(key, part):
    chosen = [4, 8, 9, 16, 18]
    grid_shape = (5, NZ, NX)
    inflow_speed = 0.1
    factor = 1.0 + 0.1 * jax.random.normal(jax.random.fold_in(key, 31), grid_shape, jnp.float32)
    levels = []
    for index in chosen:
        along = float(draw_lattice[index, 0]) * inflow_speed
        levels.append(draw_weights[index] * (1.0 + 3.0 * along + 4.5 * along * along - 1.5 * inflow_speed * inflow_speed))
    table = jnp.asarray(np.array(levels, dtype=np.float32))[:, None, None]
    return jnp.clip(table * factor, 0.005, 0.1).astype(jnp.float32)


def setup_inputs(seed: int = 0) -> dict:
    arg_keys = jax.random.split(jax.random.key(seed), 4)
    populations = draw_populations(jax.random.fold_in(arg_keys[3], 71), 0)
    solid = draw_solid(jax.random.fold_in(arg_keys[3], 71), 0)
    top_inflow = draw_top_inflow(jax.random.fold_in(arg_keys[3], 71), 0)
    return dict(populations=populations, solid=solid, top_inflow=top_inflow)


lattice = np.array([[0, 0, 0], [1, 0, 0], [-1, 0, 0], [0, 1, 0], [0, -1, 0], [0, 0, 1], [0, 0, -1],
                    [1, 1, 0], [-1, -1, 0], [1, -1, 0], [-1, 1, 0], [1, 0, 1], [-1, 0, -1],
                    [1, 0, -1], [-1, 0, 1], [0, 1, 1], [0, -1, -1], [0, 1, -1], [0, -1, 1]])
lattice_weights = [1.0 / 3.0] + [1.0 / 18.0] * 6 + [1.0 / 36.0] * 12
opposite = [0, 2, 1, 4, 3, 6, 5, 8, 7, 10, 9, 12, 11, 14, 13, 16, 15, 18, 17]
incoming = [4, 8, 9, 16, 18]
base_drive = 0.0001
drive_gain = 1.0
target_flow = 0.1


def invert_rows(matrix):
    order = len(matrix)
    work = [list(matrix[row]) + [1.0 if col == row else 0.0 for col in range(order)] for row in range(order)]
    for col in range(order):
        pivot = max(range(col, order), key=lambda row: abs(work[row][col]))
        work[col], work[pivot] = work[pivot], work[col]
        lead = work[col][col]
        work[col] = [value / lead for value in work[col]]
        for row in range(order):
            if row != col:
                factor = work[row][col]
                if factor != 0.0:
                    work[row] = [value - factor * other for value, other in zip(work[row], work[col])]
    return [line[order:] for line in work]


def collide_matrix():
    moment_rows = []
    for power in [(0, 0, 0), (1, 0, 0), (0, 1, 0), (0, 0, 1), (1, 1, 0), (1, 0, 1), (0, 1, 1),
                  (2, 0, 0), (0, 2, 0), (0, 0, 2), (1, 2, 0), (1, 0, 2), (2, 1, 0), (0, 1, 2),
                  (2, 0, 1), (0, 2, 1), (2, 2, 0), (2, 0, 2), (0, 2, 2)]:
        moment_rows.append([float(int(lattice[q, 0]) ** power[0] * int(lattice[q, 1]) ** power[1]
                                  * int(lattice[q, 2]) ** power[2]) for q in range(19)])
    rates = [0.0] * 4 + [1.8] * 6 + [1.2] * 6 + [1.1] * 3
    inverse = invert_rows(moment_rows)
    result = [[sum(inverse[row][mid] * rates[mid] * moment_rows[mid][col] for mid in range(19))
               for col in range(19)] for row in range(19)]
    return np.array(result, dtype=np.float32)


def signed_sum(populations, component):
    plus_terms = [populations[index] for index in range(19) if lattice[index, component] == 1]
    minus_terms = [populations[index] for index in range(19) if lattice[index, component] == -1]
    return reduce(lambda left, right: left + right, plus_terms) - reduce(lambda left, right: left + right, minus_terms)


def moments(populations):
    density = jnp.sum(populations, axis=0)
    momentum = (signed_sum(populations, 0), signed_sum(populations, 1), signed_sum(populations, 2))
    return density, momentum


def project(index, velocity):
    result = jnp.zeros_like(velocity[0])
    for component in range(3):
        factor = int(lattice[index, component])
        if factor == 1:
            result = result + velocity[component]
        elif factor == -1:
            result = result - velocity[component]
    return result


def equilibrium(density, velocity):
    speed_square = velocity[0] * velocity[0] + velocity[1] * velocity[1] + velocity[2] * velocity[2]
    terms = []
    for index in range(19):
        along = project(index, velocity)
        terms.append(lattice_weights[index] * density * (1.0 + 3.0 * along + 4.5 * along * along - 1.5 * speed_square))
    return jnp.stack(terms)


def collide(current, density, momentum, driving):
    velocity = tuple(part_value / density for part_value in momentum)
    base_state = equilibrium(density, velocity)
    pushed = equilibrium(density, (velocity[0] + driving / density, velocity[1], velocity[2]))
    relaxed = jnp.tensordot(jnp.asarray(collide_matrix()), current - base_state, axes=1,
                            precision=lax.Precision.HIGHEST)
    return current - relaxed + pushed - base_state


def shift_planes(carried, blocked, step_y):
    if step_y == 1:
        carried = jnp.concatenate([jnp.zeros_like(carried[:1]), carried[:-1]], axis=0)
        blocked = jnp.concatenate([jnp.ones_like(blocked[:1]), blocked[:-1]], axis=0)
    elif step_y == -1:
        carried = jnp.concatenate([carried[1:], jnp.zeros_like(carried[:1])], axis=0)
        blocked = jnp.concatenate([blocked[1:], jnp.zeros_like(blocked[:1])], axis=0)
    return carried, blocked


def stream_whole(collided, solid, top_inflow, before):
    planes = collided.shape[1]
    results = []
    for index in range(19):
        step_x = int(lattice[index, 0])
        step_y = int(lattice[index, 1])
        step_z = int(lattice[index, 2])
        carried = jnp.roll(collided[index], (step_z, step_x), axis=(1, 2))
        blocked = jnp.roll(solid, (step_z, step_x), axis=(1, 2))
        carried, blocked = shift_planes(carried, blocked, step_y)
        arrived = jnp.where(blocked == 1, collided[opposite[index]], carried)
        if step_y == -1:
            arrived = arrived.at[planes - 1].set(top_inflow[incoming.index(index)])
        results.append(arrived)
    return jnp.where(solid[None] == 1, before, jnp.stack(results))


def reference(populations, solid, top_inflow):
    fluid_nodes = (1 - solid).astype(jnp.float32)
    node_total = float(NX * NY * NZ)
    current = populations
    for step_index in range(STEPS):
        density, momentum = moments(current)
        bulk_flow = jnp.sum(momentum[0] * fluid_nodes) / node_total
        driving = base_drive + drive_gain * (target_flow - bulk_flow)
        collided = collide(current, density, momentum, driving)
        current = stream_whole(collided, solid, top_inflow, current)
    return current
```

```python
import functools

import jax
import jax.numpy as jnp
import numpy as np
from jax import lax
from jax.experimental import pallas as pl
from jax.experimental.pallas import tpu as pltpu
from jax.sharding import PartitionSpec as P

STEPS = 2
MESH = pl.DeviceIdType.MESH

lattice = np.array(
    [
        [0, 0, 0],
        [1, 0, 0],
        [-1, 0, 0],
        [0, 1, 0],
        [0, -1, 0],
        [0, 0, 1],
        [0, 0, -1],
        [1, 1, 0],
        [-1, -1, 0],
        [1, -1, 0],
        [-1, 1, 0],
        [1, 0, 1],
        [-1, 0, -1],
        [1, 0, -1],
        [-1, 0, 1],
        [0, 1, 1],
        [0, -1, -1],
        [0, 1, -1],
        [0, -1, 1],
    ]
)
CX = [int(v) for v in lattice[:, 0]]
CY = [int(v) for v in lattice[:, 1]]
CZ = [int(v) for v in lattice[:, 2]]
Q = len(CX)
weights = [1.0 / 3.0] + [1.0 / 18.0] * 6 + [1.0 / 36.0] * 12
opposite = [0, 2, 1, 4, 3, 6, 5, 8, 7, 10, 9, 12, 11, 14, 13, 16, 15, 18, 17]
incoming = [4, 8, 9, 16, 18]
base_drive = 0.0001
drive_gain = 1.0
target_flow = 0.1
RATE_TWO, RATE_ODD, RATE_FOUR = 1.8, 1.2, 1.1

X_DIRS = [[q for q in range(Q) if CX[q] == 1], [q for q in range(Q) if CX[q] == -1]]
Z_DIRS = [[q for q in range(Q) if CZ[q] == 1], [q for q in range(Q) if CZ[q] == -1]]
FACE = len(X_DIRS[0])
Z_FIELDS = FACE + 4
X_FIELDS = 3 * FACE + 1
COMBOS = [(0, 0), (1, 0), (-1, 0), (0, 1), (0, -1), (1, 1), (1, -1), (-1, 1), (-1, -1)]


def push_parts(q):
    w, cx = weights[q], CX[q]
    return (
        w * (4.5 * cx * cx - 1.5),
        3.0 * w * cx,
        9.0 * w * cx * CY[q],
        9.0 * w * cx * CZ[q],
    )


def push(q, square, drive, drive_y, drive_z):
    a, e, b, g = push_parts(q)
    value = a * square
    if e:
        value = value + e * drive
    if b:
        value = value + b * drive_y
    if g:
        value = value + g * drive_z
    return value


def push_linear(q, fields):
    a, e, b, g = push_parts(q)
    value = (2.0 * a) * fields[1] + e
    if b:
        value = value + b * fields[2]
    if g:
        value = value + g * fields[3]
    return value


def collide_base(f):
    s = {q: f[q] + f[q + 1] for q in range(1, Q, 2)}
    t = {q: f[q] - f[q + 1] for q in range(1, Q, 2)}
    plane_p, plane_q, plane_r = s[7] + s[9], s[11] + s[13], s[15] + s[17]
    axes = s[1] + s[3] + s[5]
    density = f[0] + axes + (plane_p + plane_q + plane_r)
    jx = t[1] + (t[7] + t[9]) + (t[11] + t[13])
    jy = t[3] + (t[7] - t[9]) + (t[15] + t[17])
    jz = t[5] + (t[11] - t[13]) + (t[15] - t[17])
    inverse = 1.0 / density
    ux, uy, uz = jx * inverse, jy * inverse, jz * inverse
    exx, eyy, ezz = jx * ux, jy * uy, jz * uz
    shared = density * (1.0 / 9.0) - (exx + eyy + ezz) * (1.0 / 6.0)
    hx, hy, hz = 0.5 * exx, 0.5 * eyy, 0.5 * ezz
    dp = plane_p - (shared + (hx + hy))
    dq = plane_q - (shared + (hx + hz))
    dr = plane_r - (shared + (hy + hz))
    mix = RATE_TWO - RATE_FOUR
    ax = s[1] - RATE_TWO * (s[1] - (shared + hx)) - mix * (dp + dq)
    ay = s[3] - RATE_TWO * (s[3] - (shared + hy)) - mix * (dp + dr)
    az = s[5] - RATE_TWO * (s[5] - (shared + hz)) - mix * (dq + dr)
    op, oq, orr = plane_p - RATE_FOUR * dp, plane_q - RATE_FOUR * dq, plane_r - RATE_FOUR * dr
    out = [None] * Q
    out[0] = density - ((ax + ay + az) + (op + oq + orr))
    keep = 0.5 * (1.0 - RATE_ODD)
    third, sixth = 0.5 * RATE_ODD / 3.0, 0.5 * RATE_ODD / 6.0
    for q, even, flow in ((1, ax, jx), (3, ay, jy), (5, az, jz)):
        half = 0.5 * even
        odd = keep * t[q] + third * flow
        out[q], out[q + 1] = half + odd, half - odd
    sx, sy, sz = sixth * jx, sixth * jy, sixth * jz
    for q, even, cross, one, two in (
        (7, op, jx * uy, sx, sy),
        (11, oq, jx * uz, sx, sz),
        (15, orr, jy * uz, sy, sz),
    ):
        delta = s[q] - s[q + 2]
        delta = 0.25 * (delta - RATE_TWO * (delta - cross))
        quarter = 0.25 * even
        for index, part, flow in ((q, quarter + delta, one + two), (q + 2, quarter - delta, one - two)):
            odd = keep * t[index] + flow
            out[index], out[index + 1] = part + odd, part - odd
    return out, (inverse, ux, uy, uz)


def kernel(
    sizes,
    pop_hbm,
    solid_hbm,
    inflow_hbm,
    out_ref,
    pop,
    solid_in,
    inflow,
    flags,
    masks,
    base,
    fields,
    done,
    state,
    z_send,
    z_recv,
    x_send,
    x_recv,
    a_send,
    a_recv,
    load_sem,
    z_send_sem,
    z_recv_sem,
    x_send_sem,
    x_recv_sem,
    a_send_sem,
    a_recv_sem,
):
    planes, rows, width, count_x, count_z = sizes
    total_devices = count_x * count_z
    gx, gz = lax.axis_index("gx"), lax.axis_index("gz")
    me = gx * count_z + gz

    def peer(offset):
        rank = lax.rem(me + offset, total_devices)
        return {"gx": lax.div(rank, count_z), "gz": lax.rem(rank, count_z)}

    def beside(step_x, step_z):
        return {
            "gx": lax.rem(gx + (step_x + count_x), count_x),
            "gz": lax.rem(gz + (step_z + count_z), count_z),
        }

    def each_peer(body):
        if total_devices <= 64:
            for j in range(total_devices - 1):
                body(j)
        else:

            def step(j, carry):
                body(j)
                return carry

            lax.fori_loop(0, total_devices - 1, step, 0)

    loads = [
        pltpu.make_async_copy(solid_hbm, solid_in, load_sem.at[0]),
        pltpu.make_async_copy(pop_hbm, pop, load_sem.at[1]),
        pltpu.make_async_copy(inflow_hbm, inflow, load_sem.at[2]),
    ]
    for load in loads:
        load.start()
    barrier = pltpu.get_barrier_semaphore()
    each_peer(
        lambda j: pl.semaphore_signal(barrier, inc=1, device_id=peer(j + 1), device_id_type=MESH)
    )

    lane = lax.broadcasted_iota(jnp.int32, (planes, width), 1)
    height = lax.broadcasted_iota(jnp.int32, (planes, width), 0)

    def turn(tile, shift, axis):
        shift = shift % tile.shape[axis]
        return pltpu.roll(tile, shift, axis) if shift else tile

    def strided(q, z):
        return pl.ds(q * planes * rows + z, planes, stride=rows)

    def current(step, q, z):
        return pop[strided(q, z), :] if step == 0 else state[z, q]

    def send_flow(step, acc):
        a_send[step] = jnp.sum(acc, axis=0, keepdims=True)

    def flow_copy(step, j):
        return pltpu.make_async_remote_copy(
            src_ref=a_send.at[step],
            dst_ref=a_recv.at[step, j],
            send_sem=a_send_sem.at[step],
            recv_sem=a_recv_sem.at[step],
            device_id=peer(j + 1),
            device_id_type=MESH,
        )

    def z_copy(step, side):
        return pltpu.make_async_remote_copy(
            src_ref=z_send.at[step, side],
            dst_ref=z_recv.at[step, side],
            send_sem=z_send_sem.at[step, side],
            recv_sem=z_recv_sem.at[step, side],
            device_id=beside(0, 1 - 2 * side),
            device_id_type=MESH,
        )

    def x_copy(step, side, k):
        slot = 1 - k
        return pltpu.make_async_remote_copy(
            src_ref=x_send.at[step, side],
            dst_ref=x_recv.at[step, side, slot],
            send_sem=x_send_sem.at[step, side, slot],
            recv_sem=x_recv_sem.at[step, side, slot],
            device_id=beside(1 - 2 * side, k),
            device_id_type=MESH,
        )

    x_order = [(side, k) for k in (1, -1, 0) for side in (0, 1)]

    def collide_all(step, after_edges):
        packs = [jnp.zeros((planes, width), jnp.float32) for _ in range(2)]
        order = [rows - 1, 0] + list(range(1, rows - 1))
        for place, z in enumerate(order):
            f = [current(step, q, z) for q in range(Q)]
            out, parts = collide_base(f)
            solid = flags[z + 1]
            for q in range(Q):
                base[z, q] = out[q]
            for i in range(4):
                fields[z, i] = parts[i]
            for side in range(2):
                if z == (rows - 1 if side == 0 else 0):
                    sent = [out[q] for q in Z_DIRS[side]] + [parts[0], parts[1], parts[3], solid]
                    for i, tile in enumerate(sent):
                        z_send[step, side, i] = tile
                edge = width - 1 if side == 0 else 0
                sent = [out[q] for q in X_DIRS[side]]
                sent += [push_linear(q, parts) for q in X_DIRS[side]]
                sent += [push_parts(q)[0] * parts[0] for q in X_DIRS[side]]
                sent += [solid]
                for i, tile in enumerate(sent):
                    to = i * rows + z
                    packs[side] = jnp.where(lane == to, turn(tile, to - edge, 1), packs[side])
            if place == 1:
                after_edges()
        for side in range(2):
            x_send[step, side] = packs[side]

    def x_edge(finished, side, index, row):
        slot = 0 if row < 0 else (2 if row >= rows else 1)
        at = index * rows + row % rows
        to = 0 if side == 0 else width - 1
        return turn(finished[side][slot], to - at, 1), lane == to

    def moved(tile, finished, index, row, cx):
        if cx:
            side = 0 if cx == 1 else 1
            value, where = x_edge(finished, side, index, row)
            tile = jnp.where(where, value, turn(tile, cx, 1))
        return tile

    loads[0].wait()
    for z in range(rows):
        flags[z + 1] = solid_in[pl.ds(z, planes, stride=rows), :].astype(jnp.float32)
    loads[1].wait()
    acc = jnp.zeros((planes, width), jnp.float32)
    for z in range(rows):
        plus = [pop[strided(q, z), :] for q in X_DIRS[0]]
        minus = [pop[strided(q, z), :] for q in X_DIRS[1]]
        jx = functools.reduce(lambda l, r: l + r, [p - m for p, m in zip(plus, minus)])
        acc = acc + jx * (1.0 - flags[z + 1])
    send_flow(0, acc)
    collide_all(0, lambda: None)
    loads[2].wait()
    pl.semaphore_wait(barrier, total_devices - 1)
    each_peer(lambda j: flow_copy(0, j).start())
    for side in range(2):
        z_copy(0, side).start()
    for side, k in x_order:
        x_copy(0, side, k).start()

    for step in range(STEPS):
        for side in range(2):
            z_copy(step, side).wait_recv()
        for side, k in x_order:
            x_copy(step, side, k).wait_recv()
        if step == 0:
            flags[0] = z_recv[0, 0, Z_FIELDS - 1]
            flags[rows + 1] = z_recv[0, 1, Z_FIELDS - 1]
            raw = [[x_recv[0, side, slot] for slot in range(3)] for side in range(2)]
            for row in range(-1, rows + 1):
                tile = flags[row + 1]
                for cx in (0, 1, -1):
                    shifted = moved(tile, raw, X_FIELDS - 1, row, cx)
                    for cy in (0, 1, -1):
                        if (row < 0 or row >= rows) and cx and cy:
                            continue
                        value = turn(shifted, cy, 0)
                        if cy == 1:
                            value = jnp.where(height == 0, 1.0, value)
                        elif cy == -1:
                            value = jnp.where(height == planes - 1, 0.0, value)
                        masks[row + 1, COMBOS.index((cx, cy))] = value

        pltpu.make_async_copy(a_recv.at[step], a_recv.at[step], a_recv_sem.at[step]).wait()
        flow = a_send[step] + jnp.sum(a_recv[step], axis=0)
        flow = jnp.sum(flow, axis=1, keepdims=True)
        bulk = flow / float(planes * rows * width * total_devices)
        drive = jnp.broadcast_to(base_drive + drive_gain * (target_flow - bulk), (planes, width))

        for z in range(rows):
            inverse, ux, uy, uz = (fields[z, i] for i in range(4))
            square = drive * (2.0 * ux + drive * inverse)
            drive_y, drive_z = drive * uy, drive * uz
            for q in range(Q):
                done[z + 1, q] = base[z, q] + push(q, square, drive, drive_y, drive_z)
        for side in range(2):
            row = 0 if side == 0 else rows + 1
            inverse, ux, uz = (z_recv[step, side, FACE + i] for i in range(3))
            square = drive * (2.0 * ux + drive * inverse)
            drive_z = drive * uz
            for i, q in enumerate(Z_DIRS[side]):
                done[row, q] = z_recv[step, side, i] + push(q, square, drive, None, drive_z)
        finished = []
        for side in range(2):
            tiles = []
            for slot in range(3):
                tile = x_recv[step, side, slot]
                linear = turn(tile, -FACE * rows, 1)
                second = turn(tile, -2 * FACE * rows, 1)
                tiles.append(tile + drive * (linear + drive * second))
            finished.append(tiles)

        acc = jnp.zeros((planes, width), jnp.float32)
        for z in range(rows):
            solid = flags[z + 1] > 0.5
            news = {}
            for q in range(Q):
                cx, cy, cz = CX[q], CY[q], CZ[q]
                if q == 0:
                    value = done[z + 1, 0]
                else:
                    source = z - cz
                    side = 0 if cx == 1 else 1
                    index = X_DIRS[side].index(q) if cx else None
                    value = moved(done[source + 1, q], finished, index, source, cx)
                    value = turn(value, cy, 0)
                    blocked = masks[source + 1, COMBOS.index((cx, cy))] > 0.5
                    value = jnp.where(blocked, done[z + 1, opposite[q]], value)
                    if cy == -1:
                        entering = inflow[incoming.index(q), pl.ds(z, 1), :]
                        value = jnp.where(height == planes - 1, entering, value)
                value = jnp.where(solid, current(step, q, z), value)
                if step == STEPS - 1:
                    out_ref[strided(q, z), :] = value
                else:
                    state[z, q] = value
                    news[q] = value
            if step < STEPS - 1:
                jx = functools.reduce(
                    lambda l, r: l + r, [news[p] - news[m] for p, m in zip(X_DIRS[0], X_DIRS[1])]
                )
                acc = acc + jx * (1.0 - flags[z + 1])
        if step < STEPS - 1:
            following = step + 1
            send_flow(following, acc)
            each_peer(lambda j: flow_copy(following, j).start())

            def edges():
                for side in range(2):
                    z_copy(following, side).start()

            collide_all(following, edges)
            for side, k in x_order:
                x_copy(following, side, k).start()

    for step in range(STEPS):
        for side in range(2):
            z_copy(step, side).wait_send()
        for side, k in x_order:
            x_copy(step, side, k).wait_send()
        pltpu.make_async_copy(a_recv.at[step], a_recv.at[step], a_send_sem.at[step]).wait()


def local(populations, solid, top_inflow):
    directions, planes, rows, width = populations.shape
    count_x, count_z = lax.axis_size("gx"), lax.axis_size("gz")
    assert X_FIELDS * rows <= width and count_x > 2 and count_z > 2
    devices = count_x * count_z
    tile = (planes, width)
    f32 = jnp.float32
    result = pl.pallas_call(
        functools.partial(kernel, (planes, rows, width, count_x, count_z)),
        out_shape=jax.ShapeDtypeStruct((directions * planes * rows, width), f32),
        in_specs=[pl.BlockSpec(memory_space=pl.ANY)] * 3,
        out_specs=pl.BlockSpec(memory_space=pltpu.VMEM),
        scratch_shapes=[
            pltpu.VMEM((directions * planes * rows, width), f32),
            pltpu.VMEM((planes * rows, width), jnp.int32),
            pltpu.VMEM(top_inflow.shape, f32),
            pltpu.VMEM((rows + 2,) + tile, f32),
            pltpu.VMEM((rows + 2, len(COMBOS)) + tile, f32),
            pltpu.VMEM((rows, Q) + tile, f32),
            pltpu.VMEM((rows, 4) + tile, f32),
            pltpu.VMEM((rows + 2, Q) + tile, f32),
            pltpu.VMEM((rows, Q) + tile, f32),
            pltpu.VMEM((STEPS, 2, Z_FIELDS) + tile, f32),
            pltpu.VMEM((STEPS, 2, Z_FIELDS) + tile, f32),
            pltpu.VMEM((STEPS, 2) + tile, f32),
            pltpu.VMEM((STEPS, 2, 3) + tile, f32),
            pltpu.VMEM((STEPS, 1, width), f32),
            pltpu.VMEM((STEPS, devices - 1, 1, width), f32),
            pltpu.SemaphoreType.DMA((3,)),
            pltpu.SemaphoreType.DMA((STEPS, 2)),
            pltpu.SemaphoreType.DMA((STEPS, 2)),
            pltpu.SemaphoreType.DMA((STEPS, 2, 3)),
            pltpu.SemaphoreType.DMA((STEPS, 2, 3)),
            pltpu.SemaphoreType.DMA((STEPS,)),
            pltpu.SemaphoreType.DMA((STEPS,)),
        ],
        compiler_params=pltpu.CompilerParams(
            collective_id=0, has_side_effects=True, vmem_limit_bytes=32 * 1024 * 1024
        ),
    )(
        populations.reshape(directions * planes * rows, width),
        solid.reshape(planes * rows, width),
        top_inflow,
    )
    return result.reshape(populations.shape)


def solution(mesh):
    return jax.shard_map(
        local,
        mesh=mesh,
        in_specs=(P(None, None, "gz", "gx"), P(None, "gz", "gx"), P(None, "gz", "gx")),
        out_specs=P(None, None, "gz", "gx"),
        check_vma=False,
    )
```

```python
import functools

import jax
import jax.numpy as jnp
import numpy as np
from jax import lax
from jax.experimental import pallas as pl
from jax.experimental.pallas import tpu as pltpu
from jax.sharding import PartitionSpec as P

STEPS = 2
MESH = pl.DeviceIdType.MESH

lattice = np.array(
    [
        [0, 0, 0],
        [1, 0, 0],
        [-1, 0, 0],
        [0, 1, 0],
        [0, -1, 0],
        [0, 0, 1],
        [0, 0, -1],
        [1, 1, 0],
        [-1, -1, 0],
        [1, -1, 0],
        [-1, 1, 0],
        [1, 0, 1],
        [-1, 0, -1],
        [1, 0, -1],
        [-1, 0, 1],
        [0, 1, 1],
        [0, -1, -1],
        [0, 1, -1],
        [0, -1, 1],
    ]
)
CX = [int(v) for v in lattice[:, 0]]
CY = [int(v) for v in lattice[:, 1]]
CZ = [int(v) for v in lattice[:, 2]]
Q = len(CX)
weights = [1.0 / 3.0] + [1.0 / 18.0] * 6 + [1.0 / 36.0] * 12
opposite = [0, 2, 1, 4, 3, 6, 5, 8, 7, 10, 9, 12, 11, 14, 13, 16, 15, 18, 17]
incoming = [4, 8, 9, 16, 18]
base_drive = 0.0001
drive_gain = 1.0
target_flow = 0.1
RATE_TWO, RATE_ODD, RATE_FOUR = 1.8, 1.2, 1.1

X_DIRS = [[q for q in range(Q) if CX[q] == 1], [q for q in range(Q) if CX[q] == -1]]
Z_DIRS = [[q for q in range(Q) if CZ[q] == 1], [q for q in range(Q) if CZ[q] == -1]]
FACE = len(X_DIRS[0])
Z_FIELDS = FACE + 4
X_FIELDS = 3 * FACE + 1
COMBOS = [(0, 0), (1, 0), (-1, 0), (0, 1), (0, -1), (1, 1), (1, -1), (-1, 1), (-1, -1)]


def push_parts(q):
    w, cx = weights[q], CX[q]
    return (
        w * (4.5 * cx * cx - 1.5),
        3.0 * w * cx,
        9.0 * w * cx * CY[q],
        9.0 * w * cx * CZ[q],
    )


def push(q, square, drive, drive_y, drive_z):
    a, e, b, g = push_parts(q)
    value = a * square
    if e:
        value = value + e * drive
    if b:
        value = value + b * drive_y
    if g:
        value = value + g * drive_z
    return value


def push_linear(q, fields):
    a, e, b, g = push_parts(q)
    value = (2.0 * a) * fields[1] + e
    if b:
        value = value + b * fields[2]
    if g:
        value = value + g * fields[3]
    return value


def collide_base(f):
    s = {q: f[q] + f[q + 1] for q in range(1, Q, 2)}
    t = {q: f[q] - f[q + 1] for q in range(1, Q, 2)}
    plane_p, plane_q, plane_r = s[7] + s[9], s[11] + s[13], s[15] + s[17]
    axes = s[1] + s[3] + s[5]
    density = f[0] + axes + (plane_p + plane_q + plane_r)
    jx = t[1] + (t[7] + t[9]) + (t[11] + t[13])
    jy = t[3] + (t[7] - t[9]) + (t[15] + t[17])
    jz = t[5] + (t[11] - t[13]) + (t[15] - t[17])
    inverse = 1.0 / density
    ux, uy, uz = jx * inverse, jy * inverse, jz * inverse
    exx, eyy, ezz = jx * ux, jy * uy, jz * uz
    shared = density * (1.0 / 9.0) - (exx + eyy + ezz) * (1.0 / 6.0)
    hx, hy, hz = 0.5 * exx, 0.5 * eyy, 0.5 * ezz
    dp = plane_p - (shared + (hx + hy))
    dq = plane_q - (shared + (hx + hz))
    dr = plane_r - (shared + (hy + hz))
    mix = RATE_TWO - RATE_FOUR
    ax = s[1] - RATE_TWO * (s[1] - (shared + hx)) - mix * (dp + dq)
    ay = s[3] - RATE_TWO * (s[3] - (shared + hy)) - mix * (dp + dr)
    az = s[5] - RATE_TWO * (s[5] - (shared + hz)) - mix * (dq + dr)
    op, oq, orr = plane_p - RATE_FOUR * dp, plane_q - RATE_FOUR * dq, plane_r - RATE_FOUR * dr
    out = [None] * Q
    out[0] = density - ((ax + ay + az) + (op + oq + orr))
    keep = 0.5 * (1.0 - RATE_ODD)
    third, sixth = 0.5 * RATE_ODD / 3.0, 0.5 * RATE_ODD / 6.0
    for q, even, flow in ((1, ax, jx), (3, ay, jy), (5, az, jz)):
        half = 0.5 * even
        odd = keep * t[q] + third * flow
        out[q], out[q + 1] = half + odd, half - odd
    sx, sy, sz = sixth * jx, sixth * jy, sixth * jz
    for q, even, cross, one, two in (
        (7, op, jx * uy, sx, sy),
        (11, oq, jx * uz, sx, sz),
        (15, orr, jy * uz, sy, sz),
    ):
        delta = s[q] - s[q + 2]
        delta = 0.25 * (delta - RATE_TWO * (delta - cross))
        quarter = 0.25 * even
        for index, part, flow in ((q, quarter + delta, one + two), (q + 2, quarter - delta, one - two)):
            odd = keep * t[index] + flow
            out[index], out[index + 1] = part + odd, part - odd
    return out, (inverse, ux, uy, uz)


def kernel(
    sizes,
    pop_hbm,
    solid_hbm,
    inflow_hbm,
    out_ref,
    pop,
    solid_in,
    inflow,
    flags,
    masks,
    base,
    fields,
    done,
    state,
    z_send,
    z_recv,
    x_send,
    x_recv,
    a_send,
    a_recv,
    load_sem,
    z_send_sem,
    z_recv_sem,
    x_send_sem,
    x_recv_sem,
    a_send_sem,
    a_recv_sem,
):
    planes, rows, width, count_x, count_z = sizes
    total_devices = count_x * count_z
    gx, gz = lax.axis_index("gx"), lax.axis_index("gz")
    me = gx * count_z + gz

    def peer(offset):
        rank = lax.rem(me + offset, total_devices)
        return {"gx": lax.div(rank, count_z), "gz": lax.rem(rank, count_z)}

    def beside(step_x, step_z):
        return {
            "gx": lax.rem(gx + (step_x + count_x), count_x),
            "gz": lax.rem(gz + (step_z + count_z), count_z),
        }

    def each_peer(body):
        if total_devices <= 64:
            for j in range(total_devices - 1):
                body(j)
        else:

            def step(j, carry):
                body(j)
                return carry

            lax.fori_loop(0, total_devices - 1, step, 0)

    loads = [
        pltpu.make_async_copy(solid_hbm, solid_in, load_sem.at[0]),
        pltpu.make_async_copy(pop_hbm, pop, load_sem.at[1]),
        pltpu.make_async_copy(inflow_hbm, inflow, load_sem.at[2]),
    ]
    for load in loads:
        load.start()
    barrier = pltpu.get_barrier_semaphore()
    each_peer(
        lambda j: pl.semaphore_signal(barrier, inc=1, device_id=peer(j + 1), device_id_type=MESH)
    )

    lane = lax.broadcasted_iota(jnp.int32, (planes, width), 1)
    height = lax.broadcasted_iota(jnp.int32, (planes, width), 0)

    def turn(tile, shift, axis):
        shift = shift % tile.shape[axis]
        return pltpu.roll(tile, shift, axis) if shift else tile

    def strided(q, z):
        return pl.ds(q * planes * rows + z, planes, stride=rows)

    def current(step, q, z):
        return pop[strided(q, z), :] if step == 0 else state[z, q]

    def send_flow(step, acc):
        a_send[step] = jnp.sum(acc, axis=0, keepdims=True)

    def flow_copy(step, j):
        return pltpu.make_async_remote_copy(
            src_ref=a_send.at[step],
            dst_ref=a_recv.at[step, j],
            send_sem=a_send_sem.at[step],
            recv_sem=a_recv_sem.at[step],
            device_id=peer(j + 1),
            device_id_type=MESH,
        )

    def z_copy(step, side):
        return pltpu.make_async_remote_copy(
            src_ref=z_send.at[step, side],
            dst_ref=z_recv.at[step, side],
            send_sem=z_send_sem.at[step, side],
            recv_sem=z_recv_sem.at[step, side],
            device_id=beside(0, 1 - 2 * side),
            device_id_type=MESH,
        )

    def x_copy(step, side, k):
        slot = 1 - k
        return pltpu.make_async_remote_copy(
            src_ref=x_send.at[step, side],
            dst_ref=x_recv.at[step, side, slot],
            send_sem=x_send_sem.at[step, side, slot],
            recv_sem=x_recv_sem.at[step, side, slot],
            device_id=beside(1 - 2 * side, k),
            device_id_type=MESH,
        )

    x_order = [(side, k) for k in (1, -1, 0) for side in (0, 1)]

    def collide_all(step, after_edges):
        packs = [jnp.zeros((planes, width), jnp.float32) for _ in range(2)]
        order = [rows - 1, 0] + list(range(1, rows - 1))
        for place, z in enumerate(order):
            f = [current(step, q, z) for q in range(Q)]
            out, parts = collide_base(f)
            solid = flags[z + 1]
            for q in range(Q):
                base[z, q] = out[q]
            for i in range(4):
                fields[z, i] = parts[i]
            for side in range(2):
                if z == (rows - 1 if side == 0 else 0):
                    sent = [out[q] for q in Z_DIRS[side]] + [parts[0], parts[1], parts[3], solid]
                    for i, tile in enumerate(sent):
                        z_send[step, side, i] = tile
                edge = width - 1 if side == 0 else 0
                sent = [out[q] for q in X_DIRS[side]]
                sent += [push_linear(q, parts) for q in X_DIRS[side]]
                sent += [push_parts(q)[0] * parts[0] for q in X_DIRS[side]]
                sent += [solid]
                for i, tile in enumerate(sent):
                    to = i * rows + z
                    packs[side] = jnp.where(lane == to, turn(tile, to - edge, 1), packs[side])
            if place == 1:
                after_edges()
        for side in range(2):
            x_send[step, side] = packs[side]

    def x_edge(finished, side, index, row):
        slot = 0 if row < 0 else (2 if row >= rows else 1)
        at = index * rows + row % rows
        to = 0 if side == 0 else width - 1
        return turn(finished[side][slot], to - at, 1), lane == to

    def moved(tile, finished, index, row, cx):
        if cx:
            side = 0 if cx == 1 else 1
            value, where = x_edge(finished, side, index, row)
            tile = jnp.where(where, value, turn(tile, cx, 1))
        return tile

    loads[0].wait()
    for z in range(rows):
        flags[z + 1] = solid_in[pl.ds(z, planes, stride=rows), :].astype(jnp.float32)
    loads[1].wait()
    acc = jnp.zeros((planes, width), jnp.float32)
    for z in range(rows):
        plus = [pop[strided(q, z), :] for q in X_DIRS[0]]
        minus = [pop[strided(q, z), :] for q in X_DIRS[1]]
        jx = functools.reduce(lambda l, r: l + r, [p - m for p, m in zip(plus, minus)])
        acc = acc + jx * (1.0 - flags[z + 1])
    send_flow(0, acc)
    collide_all(0, lambda: None)
    loads[2].wait()
    pl.semaphore_wait(barrier, total_devices - 1)
    each_peer(lambda j: flow_copy(0, j).start())
    for side in range(2):
        z_copy(0, side).start()
    for side, k in x_order:
        x_copy(0, side, k).start()

    for step in range(STEPS):
        for side in range(2):
            z_copy(step, side).wait_recv()
        for side, k in x_order:
            x_copy(step, side, k).wait_recv()
        if step == 0:
            flags[0] = z_recv[0, 0, Z_FIELDS - 1]
            flags[rows + 1] = z_recv[0, 1, Z_FIELDS - 1]
            raw = [[x_recv[0, side, slot] for slot in range(3)] for side in range(2)]
            for row in range(-1, rows + 1):
                tile = flags[row + 1]
                for cx in (0, 1, -1):
                    shifted = moved(tile, raw, X_FIELDS - 1, row, cx)
                    for cy in (0, 1, -1):
                        if (row < 0 or row >= rows) and cx and cy:
                            continue
                        value = turn(shifted, cy, 0)
                        if cy == 1:
                            value = jnp.where(height == 0, 1.0, value)
                        elif cy == -1:
                            value = jnp.where(height == planes - 1, 0.0, value)
                        masks[row + 1, COMBOS.index((cx, cy))] = value

        pltpu.make_async_copy(a_recv.at[step], a_recv.at[step], a_recv_sem.at[step]).wait()
        flow = a_send[step] + jnp.sum(a_recv[step], axis=0)
        flow = jnp.sum(flow, axis=1, keepdims=True)
        bulk = flow / float(planes * rows * width * total_devices)
        drive = jnp.broadcast_to(base_drive + drive_gain * (target_flow - bulk), (planes, width))

        for z in range(rows):
            inverse, ux, uy, uz = (fields[z, i] for i in range(4))
            square = drive * (2.0 * ux + drive * inverse)
            drive_y, drive_z = drive * uy, drive * uz
            for q in range(Q):
                done[z + 1, q] = base[z, q] + push(q, square, drive, drive_y, drive_z)
        for side in range(2):
            row = 0 if side == 0 else rows + 1
            inverse, ux, uz = (z_recv[step, side, FACE + i] for i in range(3))
            square = drive * (2.0 * ux + drive * inverse)
            drive_z = drive * uz
            for i, q in enumerate(Z_DIRS[side]):
                done[row, q] = z_recv[step, side, i] + push(q, square, drive, None, drive_z)
        finished = []
        for side in range(2):
            tiles = []
            for slot in range(3):
                tile = x_recv[step, side, slot]
                linear = turn(tile, -FACE * rows, 1)
                second = turn(tile, -2 * FACE * rows, 1)
                tiles.append(tile + drive * (linear + drive * second))
            finished.append(tiles)

        acc = jnp.zeros((planes, width), jnp.float32)
        for z in range(rows):
            solid = flags[z + 1] > 0.5
            news = {}
            for q in range(Q):
                cx, cy, cz = CX[q], CY[q], CZ[q]
                if q == 0:
                    value = done[z + 1, 0]
                else:
                    source = z - cz
                    side = 0 if cx == 1 else 1
                    index = X_DIRS[side].index(q) if cx else None
                    value = moved(done[source + 1, q], finished, index, source, cx)
                    value = turn(value, cy, 0)
                    blocked = masks[source + 1, COMBOS.index((cx, cy))] > 0.5
                    value = jnp.where(blocked, done[z + 1, opposite[q]], value)
                    if cy == -1:
                        entering = inflow[incoming.index(q), pl.ds(z, 1), :]
                        value = jnp.where(height == planes - 1, entering, value)
                value = jnp.where(solid, current(step, q, z), value)
                if step == STEPS - 1:
                    out_ref[strided(q, z), :] = value
                else:
                    state[z, q] = value
                    news[q] = value
            if step < STEPS - 1:
                jx = functools.reduce(
                    lambda l, r: l + r, [news[p] - news[m] for p, m in zip(X_DIRS[0], X_DIRS[1])]
                )
                acc = acc + jx * (1.0 - flags[z + 1])
        if step < STEPS - 1:
            following = step + 1
            send_flow(following, acc)
            each_peer(lambda j: flow_copy(following, j).start())

            def edges():
                for side in range(2):
                    z_copy(following, side).start()

            collide_all(following, edges)
            for side, k in x_order:
                x_copy(following, side, k).start()

    for step in range(STEPS):
        for side in range(2):
            z_copy(step, side).wait_send()
        for side, k in x_order:
            x_copy(step, side, k).wait_send()
        pltpu.make_async_copy(a_recv.at[step], a_recv.at[step], a_send_sem.at[step]).wait()


def local(populations, solid, top_inflow):
    directions, planes, rows, width = populations.shape
    count_x, count_z = lax.axis_size("gx"), lax.axis_size("gz")
    assert X_FIELDS * rows <= width and count_x > 2 and count_z > 2
    devices = count_x * count_z
    tile = (planes, width)
    f32 = jnp.float32
    result = pl.pallas_call(
        functools.partial(kernel, (planes, rows, width, count_x, count_z)),
        out_shape=pltpu.VMEM((directions * planes * rows, width), f32),
        in_specs=[pl.BlockSpec(memory_space=pltpu.HBM)] * 3,
        out_specs=pl.BlockSpec(memory_space=pltpu.VMEM),
        scratch_shapes=[
            pltpu.VMEM((directions * planes * rows, width), f32),
            pltpu.VMEM((planes * rows, width), jnp.int32),
            pltpu.VMEM(top_inflow.shape, f32),
            pltpu.VMEM((rows + 2,) + tile, f32),
            pltpu.VMEM((rows + 2, len(COMBOS)) + tile, f32),
            pltpu.VMEM((rows, Q) + tile, f32),
            pltpu.VMEM((rows, 4) + tile, f32),
            pltpu.VMEM((rows + 2, Q) + tile, f32),
            pltpu.VMEM((rows, Q) + tile, f32),
            pltpu.VMEM((STEPS, 2, Z_FIELDS) + tile, f32),
            pltpu.VMEM((STEPS, 2, Z_FIELDS) + tile, f32),
            pltpu.VMEM((STEPS, 2) + tile, f32),
            pltpu.VMEM((STEPS, 2, 3) + tile, f32),
            pltpu.VMEM((STEPS, 1, width), f32),
            pltpu.VMEM((STEPS, devices - 1, 1, width), f32),
            pltpu.SemaphoreType.DMA((3,)),
            pltpu.SemaphoreType.DMA((STEPS, 2)),
            pltpu.SemaphoreType.DMA((STEPS, 2)),
            pltpu.SemaphoreType.DMA((STEPS, 2, 3)),
            pltpu.SemaphoreType.DMA((STEPS, 2, 3)),
            pltpu.SemaphoreType.DMA((STEPS,)),
            pltpu.SemaphoreType.DMA((STEPS,)),
        ],
        compiler_params=pltpu.CompilerParams(
            collective_id=0, has_side_effects=True, vmem_limit_bytes=60_000_000
        ),
    )(
        populations.reshape(directions * planes * rows, width),
        solid.reshape(planes * rows, width),
        top_inflow,
    )
    return result.reshape(populations.shape)


def solution(mesh):
    return jax.shard_map(
        local,
        mesh=mesh,
        in_specs=(P(None, None, "gz", "gx"), P(None, "gz", "gx"), P(None, "gz", "gx")),
        out_specs=P(None, None, "gz", "gx"),
        check_vma=False,
    )
```
